256 devices in a mesh: dp: 8 (over z), task: 16 (over y, x), mp: 2 (over core).
Axes of the slice: x: 4, y: 4, z: 8, core: 2. Of those that a mesh axis runs over, the one named last changes fastest.
Arguments:
- deltas: bfloat16 [16, 2, 256, 28672], P('task', None, 'dp', 'mp'), may hold values from -3.984375 to 3.984375, as said below
- keep_blocks: int32 [16, 2, 2], P('task'), may hold values 0 or 1
- base_weights: bfloat16 [2, 256, 28672], P(None, 'dp', 'mp'), may hold values from -6 to 6
Outputs:
- merged: float32 [2, 256, 28672], P(None, 'dp', 'mp')
The draws below stay inside these ranges and needn't reach their ends.
Inputs may be any that keep to these rules, and one draw needn't show every extreme that they name: `deltas`: every entry is a whole multiple of 1/64.
All inputs are finite; a program needn't handle non-finite values. No bound on the sum of `keep_blocks` on one device may be relied on, other than what follows from the above.
Results may differ from the reference program's by a relative error of at most 0.0003.
Values may be sent and summed in bfloat16 or wider, within the bound.
A program may use at most 128 MiB of HBM per device.

```python
import jax
import jax.numpy as jnp

FF = 28672
BLOCK = 128
ROWS = 256
BLOCKS = 2
TASKS = 16


def draw_deltas(key, part):
    shape = (TASKS, 2, ROWS, FF)
    first_key, second_key = jax.random.split(jax.random.fold_in(key, 17))
    level = jax.random.randint(first_key, shape, -128, 129) + jax.random.randint(second_key, shape, -127, 128)
    return (level.astype(jnp.float32) / 64.0).astype(jnp.bfloat16)


def place_ends(entries, stream_key, least, high):
    index_at = [jax.random.randint(jax.random.fold_in(stream_key, axis), (), 0, length) for axis, length in enumerate(entries.shape)]
    widest = entries.shape.index(max(entries.shape))
    neighbour = index_at[:widest] + [(index_at[widest] + 1) % entries.shape[widest]] + index_at[widest + 1:]
    return entries.at[tuple(index_at)].set(least).at[tuple(neighbour)].set(high)


def block_levels(own_key, shape, pieces, least, high):
    def one(position, parts):
        heights = jax.random.uniform(jax.random.fold_in(jax.random.fold_in(own_key, 6), position), (parts,), jnp.float32, least / len(pieces), high / len(pieces))
        return jnp.repeat(jnp.exp(heights), shape[position] // parts).reshape((-1,) + (1,) * (len(shape) - position - 1))

    loudness = one(*pieces[0])
    for cut in pieces[1:]:
        loudness = loudness * one(*cut)
    return loudness


def centred(stream_key, extent, deviation, most, cuts=(), dtype=jnp.bfloat16):
    loudness = block_levels(stream_key, extent, cuts, -0.22, 0.18) if cuts else 1.0
    values = jax.random.normal(stream_key, extent, jnp.float32) * deviation * loudness
    return jnp.minimum(jnp.maximum(values, -most), most).astype(dtype)


def setup_inputs(seed: int = 0) -> dict:
    keys = jax.random.split(jax.random.key(seed), 4)
    deltas = draw_deltas(jax.random.fold_in(keys[3], 71), 0)
    keep_blocks = place_ends((jax.random.randint(keys[1], (TASKS, 2, BLOCKS), 0, 2) < 1).astype(jnp.int32), jax.random.fold_in(keys[1], 1), 0, 1)
    base_weights = centred(keys[2], (2, ROWS, FF), 1.0, 6.0, ((1, 8), (2, 2)))
    return dict(deltas=deltas, keep_blocks=keep_blocks, base_weights=base_weights)


def reference(deltas, keep_blocks, base_weights):
    row_keep = jnp.repeat(keep_blocks, BLOCK, axis=2).astype(jnp.float32)
    shape = base_weights.shape
    upward = jnp.zeros(shape, jnp.float32)
    downward = jnp.zeros(shape, jnp.float32)
    up_count = jnp.zeros(shape, jnp.float32)
    down_count = jnp.zeros(shape, jnp.float32)
    for which in range(TASKS):
        trimmed = deltas[which].astype(jnp.float32) * row_keep[which][:, :, None]
        upward = upward + jnp.maximum(trimmed, 0.0)
        downward = downward + jnp.minimum(trimmed, 0.0)
        up_count = up_count + (trimmed > 0).astype(jnp.float32)
        down_count = down_count + (trimmed < 0).astype(jnp.float32)
    elected = jnp.sign(upward + downward)
    upper_mean = upward / jnp.maximum(up_count, 1.0)
    lower_mean = downward / jnp.maximum(down_count, 1.0)
    agreed = jnp.where(elected > 0, upper_mean, jnp.where(elected < 0, lower_mean, 0.0))
    return base_weights.astype(jnp.float32) + agreed
```

```python
import functools

import jax
import jax.numpy as jnp
from jax import lax
from jax.experimental import pallas as pl
from jax.experimental.pallas import tpu as pltpu
from jax.sharding import PartitionSpec as P

BLOCK = 128
SIDE = 4
TASKS = SIDE * SIDE
MESH = pl.DeviceIdType.MESH

CHUNKS = (384, 384, 128)
FAR_FIRST = (
    (2, 2), (2, 1), (1, 2), (2, 3), (3, 2), (1, 1), (3, 3), (1, 3), (3, 1),
    (0, 2), (2, 0), (0, 1), (1, 0), (0, 3), (3, 0),
)


def fraction_table(shape):
    j = lax.broadcasted_iota(jnp.int32, shape, 1)
    n = jnp.zeros(shape, jnp.int32)
    for m in range(1, 17):
        n = n + jnp.where(j >= m * (m - 1) // 2, 1, 0)
    r = j - n * (n - 1) // 2
    r = jnp.where(n == 16, 2 * r + 1, r)
    return r.astype(jnp.float32) / n.astype(jnp.float32)


def encode(upward, downward, up_count, down_count):
    total = upward + downward
    positive = total > 0.0
    amount = jnp.where(positive, upward, -downward) * 64.0
    count = jnp.where(positive, up_count, down_count) * 64.0
    n = jnp.maximum(count, 1.0)
    whole = jnp.floor(amount / n + 0.015625)
    r = amount - whole * n
    half = jnp.floor(r * 0.5)
    odd = r - 2.0 * half
    slot = n * (n - 1.0) * 0.5 + r
    slot16 = jnp.where(odd > 0.0, 120.0 + half, 28.0 + half)
    slot = jnp.where(n > 15.5, slot16, slot)
    code = whole * 128.0 + slot
    code = jnp.where(positive, code, jnp.where(total < 0.0, -code, 0.0))
    return code.astype(jnp.int32).astype(jnp.int16)


def decode(code, table):
    c = code.astype(jnp.int32)
    a = jnp.abs(c)
    whole = lax.shift_right_logical(a, 7).astype(jnp.float32)
    part = jnp.take_along_axis(table, a & 127, axis=1)
    mean = (whole + part) * 0.015625
    return jnp.where(c < 0, -mean, mean)


def kernel(chunks, keep_ref, deltas_ref, base_ref, out_ref, own, base, *scratch):
    kinds = len(chunks)
    arrived = scratch[:kinds]
    codes = scratch[kinds : 2 * kinds]
    load_sem, send_sem, recv_sem = scratch[2 * kinds :]
    rows, columns = own.shape[1], own.shape[2]
    share = columns // TASKS
    task = lax.axis_index("task")
    y, x = task // SIDE, task % SIDE
    block = lax.axis_index("dp") * rows // BLOCK

    def at(dy, dx):
        return (y + dy) % SIDE * SIDE + (x + dx) % SIDE

    loads = [
        pltpu.make_async_copy(deltas_ref.at[0, p], own.at[p], load_sem.at[p]) for p in range(2)
    ]
    base_load = pltpu.make_async_copy(base_ref, base, load_sem.at[2])
    for load in loads:
        load.start()
    base_load.start()

    barrier = pltpu.get_barrier_semaphore()
    for dy, dx in FAR_FIRST:
        pl.semaphore_signal(barrier, inc=1, device_id={"task": at(dy, dx)}, device_id_type=MESH)

    step = columns // 8
    for p in range(2):
        loads[p].wait()
        keep = keep_ref[0, p, block].astype(jnp.float32)

        @pl.loop(0, 8)
        def _(i):
            part = pl.ds(pl.multiple_of(i * step, 128), step)
            own[p, :, part] = (own[p, :, part].astype(jnp.float32) * keep).astype(jnp.bfloat16)

    pl.semaphore_wait(barrier, len(FAR_FIRST))

    sent = []

    def send(src, dst, dy, dx):
        i = len(sent)
        copy = pltpu.make_async_remote_copy(
            src_ref=src,
            dst_ref=dst,
            send_sem=send_sem.at[i],
            recv_sem=recv_sem.at[i],
            device_id={"task": at(dy, dx)},
            device_id_type=MESH,
        )
        copy.start()
        sent.append(copy)
        return copy

    starts = [sum(chunks[:k]) for k in range(kinds)]

    def lanes(of_task, k, off=0, width=None):
        start = pl.multiple_of(of_task * share + starts[k] + off, 128)
        return pl.ds(start, width or chunks[k])

    exchange = [
        [
            send(own.at[:, :, lanes(at(dy, dx), k)], arrived[k].at[i], dy, dx)
            for i, (dy, dx) in enumerate(FAR_FIRST)
        ]
        for k in range(kinds)
    ]

    def reduce(k):
        for copy in exchange[k]:
            copy.wait_recv()
        width = chunks[k]
        tile = 128
        for p in range(2):
            for off in range(0, width, tile):
                zero = jnp.zeros((rows, tile), jnp.float32)
                upward = downward = up_count = down_count = zero
                for source in range(TASKS):
                    if source < TASKS - 1:
                        value = arrived[k][source, p, :, off : off + tile]
                    else:
                        value = own[p, :, lanes(task, k, off, tile)]
                    value = value.astype(jnp.float32)
                    up, down = jnp.maximum(value, 0.0), jnp.minimum(value, 0.0)
                    upward, downward = upward + up, downward + down
                    up_count = up_count + jnp.minimum(up, 0.015625)
                    down_count = down_count - jnp.maximum(down, -0.015625)
                codes[k][p, task, :, off : off + tile] = encode(upward, downward, up_count, down_count)

    def turn(p, first, second):
        return (second, first) if p == 0 else (first, second)

    def piece(k, p, first, second):
        return codes[k].at[p, at(*turn(p, first, second))]

    def pass_on(k, p, first, second, to_first, to_second):
        ref = piece(k, p, first, second)
        return send(ref, ref, *turn(p, to_first, to_second))

    def first_stage(k):
        return [{d: pass_on(k, p, 0, 0, d, 0) for d in (1, 3, 2)} for p in range(2)]

    def second_stage(k, line, got):
        for d in (0, 3, 1, 2):
            for p in range(2):
                if d:
                    line[p][4 - d].wait_recv()
                for e in (1, 3):
                    got[p][d, e] = pass_on(k, p, d, 0, 0, e)

    def third_stage(k, got, last):
        for d, e in ((0, 1), (3, 3), (1, 1), (2, 3)):
            for p in range(2):
                got[p][d, e].wait_recv()
                last[p][d] = pass_on(k, p, d, 4 - e, 0, e)
        for d, e in ((0, 3), (3, 1), (1, 3), (2, 1)):
            for p in range(2):
                got[p][d, e].wait_recv()

    table = fraction_table((rows, 128))

    def decode_piece(k, p, first, second):
        of_task = at(*turn(p, first, second))
        for off in range(0, chunks[k], 128):
            where = lanes(of_task, k, off, 128)
            mean = decode(codes[k][p, of_task, :, off : off + 128], table)
            out_ref[p, :, where] = base[p, :, where].astype(jnp.float32) + mean

    lines, gots, lasts = [], [], []
    for k in range(kinds):
        reduce(k)
        lines.append(first_stage(k))
        gots.append([{}, {}])
        lasts.append([{}, {}])
        if k > 0:
            second_stage(k - 1, lines[k - 1], gots[k - 1])
    second_stage(kinds - 1, lines[-1], gots[-1])
    base_load.wait()
    for k in range(kinds):
        third_stage(k, gots[k], lasts[k])
        for p in range(2):
            for d in range(4):
                for e in (0, 1, 3):
                    decode_piece(k, p, d, e)
    for k in range(kinds):
        for p in range(2):
            for d in range(4):
                lasts[k][p][d].wait_recv()
                decode_piece(k, p, d, 2)
    for copy in sent:
        copy.wait_send()


def on_device(deltas, keep_blocks, base_weights):
    halves, rows, columns = base_weights.shape
    share = columns // TASKS
    assert sum(CHUNKS) == share
    copies = len(CHUNKS) * 45
    return pl.pallas_call(
        functools.partial(kernel, CHUNKS),
        out_shape=jax.ShapeDtypeStruct((halves, rows, columns), jnp.float32),
        in_specs=[
            pl.BlockSpec(memory_space=pltpu.SMEM),
            pl.BlockSpec(memory_space=pltpu.HBM),
            pl.BlockSpec(memory_space=pltpu.HBM),
        ],
        out_specs=pl.BlockSpec(memory_space=pltpu.VMEM),
        scratch_shapes=[
            pltpu.VMEM((halves, rows, columns), jnp.bfloat16),
            pltpu.VMEM((halves, rows, columns), jnp.bfloat16),
            *[pltpu.VMEM((TASKS - 1, halves, rows, width), jnp.bfloat16) for width in CHUNKS],
            *[pltpu.VMEM((halves, TASKS, rows, width), jnp.int16) for width in CHUNKS],
            pltpu.SemaphoreType.DMA((3,)),
            pltpu.SemaphoreType.DMA((copies,)),
            pltpu.SemaphoreType.DMA((copies,)),
        ],
        compiler_params=pltpu.CompilerParams(
            collective_id=0, has_side_effects=True, vmem_limit_bytes=40 * 2**20
        ),
        name="merge",
    )(keep_blocks, deltas, base_weights)


def solution(mesh):
    in_specs = (P("task", None, "dp", "mp"), P("task", None, None), P(None, "dp", "mp"))
    out_specs = P(None, "dp", "mp")
    return jax.shard_map(
        on_device, mesh=mesh, in_specs=in_specs, out_specs=out_specs, check_vma=False
    )
```

```python
import functools

import jax
import jax.numpy as jnp
from jax import lax
from jax.experimental import pallas as pl
from jax.experimental.pallas import tpu as pltpu
from jax.sharding import PartitionSpec as P

BLOCK = 128
SIDE = 4
TASKS = SIDE * SIDE
MESH = pl.DeviceIdType.MESH

CHUNKS = (384, 384, 128)
FAR_FIRST = (
    (2, 2), (2, 1), (1, 2), (2, 3), (3, 2), (1, 1), (3, 3), (1, 3), (3, 1),
    (0, 2), (2, 0), (0, 1), (1, 0), (0, 3), (3, 0),
)

GROUPS = 5


def fraction_table(shape):
    j = lax.broadcasted_iota(jnp.int32, shape, 1)
    n = jnp.zeros(shape, jnp.int32)
    for m in range(1, 17):
        n = n + jnp.where(j >= m * (m - 1) // 2, 1, 0)
    r = j - n * (n - 1) // 2
    r = jnp.where(n == 16, 2 * r + 1, r)
    return r.astype(jnp.float32) / n.astype(jnp.float32)


def encode(upward, downward, up_count, down_count):
    total = upward + downward
    positive = total > 0.0
    amount = jnp.where(positive, upward, -downward) * 64.0
    count = jnp.where(positive, up_count, down_count) * 64.0
    n = jnp.maximum(count, 1.0)
    whole = jnp.floor(amount / n + 0.015625)
    r = amount - whole * n
    half = jnp.floor(r * 0.5)
    odd = r - 2.0 * half
    slot = n * (n - 1.0) * 0.5 + r
    slot16 = jnp.where(odd > 0.0, 120.0 + half, 28.0 + half)
    slot = jnp.where(n > 15.5, slot16, slot)
    code = whole * 128.0 + slot
    code = jnp.where(positive, code, jnp.where(total < 0.0, -code, 0.0))
    return code.astype(jnp.int32).astype(jnp.int16)


def decode(code, table):
    c = code.astype(jnp.int32)
    a = jnp.abs(c)
    whole = lax.shift_right_logical(a, 7).astype(jnp.float32)
    part = jnp.take_along_axis(table, a & 127, axis=1)
    mean = (whole + part) * 0.015625
    return jnp.where(c < 0, -mean, mean)


def kernel(chunks, keep_hbm, deltas_ref, base_ref, out_ref, own, base, keep_ref, keep_sem, *scratch):
    kinds = len(chunks)
    arrived = scratch[:kinds]
    codes = scratch[kinds : 2 * kinds]
    load_sem, send_sem, recv_sem = scratch[2 * kinds :]
    rows, columns = own.shape[1], own.shape[2]
    share = columns // TASKS
    task = lax.axis_index("task")
    y, x = task // SIDE, task % SIDE
    block = lax.axis_index("dp") * rows // BLOCK

    def at(dy, dx):
        return (y + dy) % SIDE * SIDE + (x + dx) % SIDE

    loads = [
        pltpu.make_async_copy(deltas_ref.at[0, p], own.at[p], load_sem.at[p]) for p in range(2)
    ]
    base_load = pltpu.make_async_copy(base_ref, base, load_sem.at[2])
    for load in loads:
        load.start()
    base_load.start()
    keep_load = pltpu.make_async_copy(keep_hbm, keep_ref, keep_sem)
    keep_load.start()

    barrier = pltpu.get_barrier_semaphore()
    for dy, dx in FAR_FIRST:
        pl.semaphore_signal(barrier, inc=1, device_id={"task": at(dy, dx)}, device_id_type=MESH)

    step = columns // 8
    keep_load.wait()
    for p in range(2):
        loads[p].wait()
        keep = keep_ref[0, p, block].astype(jnp.float32)

        @pl.loop(0, 8)
        def _(i):
            part = pl.ds(pl.multiple_of(i * step, 128), step)
            own[p, :, part] = (own[p, :, part].astype(jnp.float32) * keep).astype(jnp.bfloat16)

    pl.semaphore_wait(barrier, len(FAR_FIRST))

    def send(src, dst, pair, dy, dx):
        copy = pltpu.make_async_remote_copy(
            src_ref=src,
            dst_ref=dst,
            send_sem=pair[0],
            recv_sem=pair[1],
            device_id={"task": at(dy, dx)},
            device_id_type=MESH,
        )
        copy.start()

    def wait(ref, sem):
        pltpu.make_async_copy(ref, ref, sem).wait()

    starts = [sum(chunks[:k]) for k in range(kinds)]

    def lanes(of_task, k, off=0, width=None):
        start = pl.multiple_of(of_task * share + starts[k] + off, 128)
        return pl.ds(start, width or chunks[k])

    for k in range(kinds):
        for i, (dy, dx) in enumerate(FAR_FIRST):
            pair = (send_sem.at[k, 0], recv_sem.at[k, 0])
            send(own.at[:, :, lanes(at(dy, dx), k)], arrived[k].at[i], pair, dy, dx)

    def reduce(k):
        wait(arrived[k], recv_sem.at[k, 0])
        width = chunks[k]
        tile = 128
        for p in range(2):
            for off in range(0, width, tile):
                zero = jnp.zeros((rows, tile), jnp.float32)
                upward = downward = up_count = down_count = zero
                for source in range(TASKS):
                    if source < TASKS - 1:
                        value = arrived[k][source, p, :, off : off + tile]
                    else:
                        value = own[p, :, lanes(task, k, off, tile)]
                    value = value.astype(jnp.float32)
                    up, down = jnp.maximum(value, 0.0), jnp.minimum(value, 0.0)
                    upward, downward = upward + up, downward + down
                    up_count = up_count + jnp.minimum(up, 0.015625)
                    down_count = down_count - jnp.maximum(down, -0.015625)
                codes[k][p, task, :, off : off + tile] = encode(upward, downward, up_count, down_count)

    def turn(p, first, second):
        return (second, first) if p == 0 else (first, second)

    def piece(k, p, first, second):
        return codes[k].at[p, at(*turn(p, first, second))]

    def pass_on(k, p, group, first, second, to_first, to_second):
        ref = piece(k, p, first, second)
        pair = (send_sem.at[k, 1], recv_sem.at[k, 1 + GROUPS * p + group])
        send(ref, ref, pair, *turn(p, to_first, to_second))

    def wait_pieces(k, p, group, count):
        wait(codes[k].at[p, pl.ds(0, count)], recv_sem.at[k, 1 + GROUPS * p + group])

    def first_stage(k):
        for p in range(2):
            for d in (1, 3, 2):
                pass_on(k, p, d // 2 * (3 - d), 0, 0, d, 0)

    def second_stage(k):
        for d in (0, 3, 1, 2):
            for p in range(2):
                if d == 3:
                    wait_pieces(k, p, 0, 2)
                if d == 2:
                    wait_pieces(k, p, 1, 1)
                for e in (1, 3):
                    group = 2 if (e == 1) == (d < 2) else 3
                    pass_on(k, p, group, d, 0, 0, e)

    def third_stage(k):
        for p in range(2):
            wait_pieces(k, p, 2, 4)
            for d in range(4):
                e = 1 if d < 2 else 3
                pass_on(k, p, 4, d, 4 - e, 0, e)

    table = fraction_table((rows, 128))

    def decode_piece(k, p, first, second):
        of_task = at(*turn(p, first, second))
        for off in range(0, chunks[k], 128):
            where = lanes(of_task, k, off, 128)
            mean = decode(codes[k][p, of_task, :, off : off + 128], table)
            out_ref[p, :, where] = base[p, :, where].astype(jnp.float32) + mean

    for k in range(kinds):
        reduce(k)
        first_stage(k)
        if k > 0:
            second_stage(k - 1)
    second_stage(kinds - 1)
    base_load.wait()
    for k in range(kinds):
        third_stage(k)
        for p in range(2):
            wait_pieces(k, p, 3, 4)
            for d in range(4):
                for e in (0, 1, 3):
                    decode_piece(k, p, d, e)
    for k in range(kinds):
        for p in range(2):
            wait_pieces(k, p, 4, 4)
            for d in range(4):
                decode_piece(k, p, d, 2)
    for k in range(kinds):
        wait(arrived[k], send_sem.at[k, 0])
        wait(codes[k].at[:, pl.ds(0, TASKS - 1)], send_sem.at[k, 1])


def on_device(deltas, keep_blocks, base_weights):
    halves, rows, columns = base_weights.shape
    share = columns // TASKS
    assert sum(CHUNKS) == share
    operands = [
        pltpu.with_memory_space_constraint(value, pltpu.HBM)
        for value in (keep_blocks, deltas, base_weights)
    ]
    return pl.pallas_call(
        functools.partial(kernel, CHUNKS),
        out_shape=jax.ShapeDtypeStruct((halves, rows, columns), jnp.float32),
        in_specs=[
            pl.BlockSpec(memory_space=pltpu.HBM),
            pl.BlockSpec(memory_space=pltpu.HBM),
            pl.BlockSpec(memory_space=pltpu.HBM),
        ],
        out_specs=pl.BlockSpec(memory_space=pltpu.VMEM),
        scratch_shapes=[
            pltpu.VMEM((halves, rows, columns), jnp.bfloat16),
            pltpu.VMEM((halves, rows, columns), jnp.bfloat16),
            pltpu.SMEM(keep_blocks.shape, jnp.int32),
            pltpu.SemaphoreType.DMA,
            *[pltpu.VMEM((TASKS - 1, halves, rows, width), jnp.bfloat16) for width in CHUNKS],
            *[pltpu.VMEM((halves, TASKS, rows, width), jnp.int16) for width in CHUNKS],
            pltpu.SemaphoreType.DMA((3,)),
            pltpu.SemaphoreType.DMA((len(CHUNKS), 2)),
            pltpu.SemaphoreType.DMA((len(CHUNKS), 1 + 2 * GROUPS)),
        ],
        compiler_params=pltpu.CompilerParams(
            collective_id=0, has_side_effects=True, vmem_limit_bytes=40 * 2**20
        ),
        name="merge",
    )(*operands)


def solution(mesh):
    in_specs = (P("task", None, "dp", "mp"), P("task", None, None), P(None, "dp", "mp"))
    out_specs = P(None, "dp", "mp")
    return jax.shard_map(
        on_device, mesh=mesh, in_specs=in_specs, out_specs=out_specs, check_vma=False
    )
```

```python
import functools

import jax
import jax.numpy as jnp
from jax import lax
from jax.experimental import pallas as pl
from jax.experimental.pallas import tpu as pltpu
from jax.sharding import PartitionSpec as P

BLOCK = 128
SIDE = 4
TASKS = SIDE * SIDE
MESH = pl.DeviceIdType.MESH

CHUNKS = (256, 256, 256, 128)
HALF = 16
PEERS = ((0, 2), (2, 0), (0, 1), (1, 0), (0, 3), (3, 0))
SENDS, RECEIVES = 3, 9


def fraction_table(shape):
    j = lax.broadcasted_iota(jnp.int32, shape, 1)
    n = jnp.zeros(shape, jnp.int32)
    for m in range(1, 17):
        n = n + jnp.where(j >= m * (m - 1) // 2, 1, 0)
    r = j - n * (n - 1) // 2
    r = jnp.where(n == 16, 2 * r + 1, r)
    return r.astype(jnp.float32) / n.astype(jnp.float32)


def encode(upward, downward, up_count, down_count):
    total = upward + downward
    positive = total > 0.0
    amount = jnp.where(positive, upward, -downward) * 64.0
    count = jnp.where(positive, up_count, down_count) * 64.0
    n = jnp.maximum(count, 1.0)
    whole = jnp.floor(amount / n + 0.015625)
    r = amount - whole * n
    half = jnp.floor(r * 0.5)
    odd = r - 2.0 * half
    slot = n * (n - 1.0) * 0.5 + r
    slot16 = jnp.where(odd > 0.0, 120.0 + half, 28.0 + half)
    slot = jnp.where(n > 15.5, slot16, slot)
    code = whole * 128.0 + slot
    code = jnp.where(positive, code, jnp.where(total < 0.0, -code, 0.0))
    return code.astype(jnp.int32).astype(jnp.int16)


def decode(code, table):
    c = code.astype(jnp.int32)
    a = jnp.abs(c)
    whole = lax.shift_right_logical(a, 7).astype(jnp.float32)
    part = jnp.take_along_axis(table, a & 127, axis=1)
    mean = (whole + part) * 0.015625
    return jnp.where(c < 0, -mean, mean)


def tally(values, totals=None):
    for value in values:
        value = value.astype(jnp.float32)
        up, down = jnp.maximum(value, 0.0), jnp.minimum(value, 0.0)
        new = (up, down, jnp.minimum(up, 0.015625), -jnp.maximum(down, -0.015625))
        totals = new if totals is None else tuple(a + b for a, b in zip(totals, new))
    return totals


def kernel(chunks, keep_hbm, deltas_ref, base_ref, out_ref, own, base, keep_ref, load_sem, send_sem, recv_sem, *scratch):
    kinds = len(chunks)
    bundles, line, transit, direct, merged, partial, codes = (
        scratch[i * kinds : (i + 1) * kinds] for i in range(7)
    )
    rows, columns = own.shape[1], own.shape[2]
    share = columns // TASKS
    task = lax.axis_index("task")
    y, x = task // SIDE, task % SIDE
    block = lax.axis_index("dp") * rows // BLOCK
    halves = (slice(0, HALF), slice(HALF, rows))

    def at(dy, dx):
        return (y + dy) % SIDE * SIDE + (x + dx) % SIDE

    def turn(p, first, second):
        return (second, first) if p == 0 else (first, second)

    def place(p, second):
        return ((y, x)[p] + second) % SIDE

    keep_load = pltpu.make_async_copy(keep_hbm, keep_ref, load_sem.at[3])
    keep_load.start()
    loads = [
        pltpu.make_async_copy(deltas_ref.at[0, p], own.at[p], load_sem.at[p]) for p in range(2)
    ]
    base_load = pltpu.make_async_copy(base_ref, base, load_sem.at[2])
    for load in loads:
        load.start()
    base_load.start()

    barrier = pltpu.get_barrier_semaphore()
    for dy, dx in PEERS:
        pl.semaphore_signal(barrier, inc=1, device_id={"task": at(dy, dx)}, device_id_type=MESH)
    keep_load.wait()
    keeps = [keep_ref[0, p, block].astype(jnp.float32) for p in range(2)]

    def send(src, dst, k, send_slot, recv_slot, p, first, second):
        dy, dx = turn(p, first, second)
        pltpu.make_async_remote_copy(
            src_ref=src,
            dst_ref=dst,
            send_sem=send_sem.at[k, send_slot],
            recv_sem=recv_sem.at[k, recv_slot],
            device_id={"task": at(dy, dx)},
            device_id_type=MESH,
        ).start()

    def wait(ref, sem):
        pltpu.make_async_copy(ref, ref, sem).wait()

    starts = [sum(chunks[:k]) for k in range(kinds)]

    def lanes(of_task, k, off=0, width=None):
        start = pl.multiple_of(of_task * share + starts[k] + off, 128)
        return pl.ds(start, width or chunks[k])

    def trim(k):
        for d in (2, 1, 3, 0):
            for p in range(2):
                for q in range(SIDE):
                    first = ((x, y)[p] + d) % SIDE
                    of_task = q * SIDE + first if p == 0 else first * SIDE + q
                    value = own[p, :, lanes(of_task, k)].astype(jnp.float32) * keeps[p]
                    if d:
                        bundles[k][p, d - 1, q] = value.astype(jnp.bfloat16)
                    else:
                        line[k][p, 0, q] = value.astype(jnp.bfloat16)

    def send_bundles(k):
        for d in (2, 1, 3):
            for p in range(2):
                send(bundles[k].at[p, d - 1], line[k].at[p, d], k, 0, 0, p, d, 0)

    def send_transit(k):
        wait(line[k].at[:, pl.ds(1, 3)], recv_sem.at[k, 0])
        for side, e in ((0, 1), (1, 3)):
            for p in range(2):
                far = line[k].at[p, :, place(p, 2), halves[side]]
                send(far, transit[k].at[p, side], k, 1, 1, p, 0, e)

    def send_direct(k):
        for side, e in ((0, 1), (1, 3)):
            for p in range(2):
                near = line[k].at[p, :, place(p, e), halves[1 - side]]
                send(near, direct[k].at[p, side], k, 1, 2, p, 0, e)

    def merge(k):
        wait(transit[k], recv_sem.at[k, 1])
        for side, e in ((0, 1), (1, 3)):
            for p in range(2):
                for off in range(0, chunks[k], 128):
                    tile = slice(off, off + 128)
                    values = [transit[k][p, side, j, :, tile] for j in range(SIDE)]
                    values += [line[k][p, j, place(p, e), halves[side], tile] for j in range(SIDE)]
                    for i, total in enumerate(tally(values)):
                        total = (total * 64.0).astype(jnp.int32).astype(jnp.int16)
                        merged[k][p, side, i, :, tile] = total
        for side, e in ((0, 1), (1, 3)):
            for p in range(2):
                send(merged[k].at[p, side], partial[k].at[p, side], k, 1, 3, p, 0, e)

    def reduce(k):
        wait(direct[k], recv_sem.at[k, 2])
        wait(partial[k], recv_sem.at[k, 3])
        for p in range(2):
            for side in range(2):
                for off in range(0, chunks[k], 128):
                    tile = slice(off, off + 128)
                    totals = tuple(
                        partial[k][p, side, i, :, tile].astype(jnp.int32).astype(jnp.float32) * 0.015625
                        for i in range(4)
                    )
                    values = [direct[k][p, 1 - side, j, :, tile] for j in range(SIDE)]
                    values += [line[k][p, j, place(p, 0), halves[side], tile] for j in range(SIDE)]
                    codes[k][p, task, halves[side], tile] = encode(*tally(values, totals))

    def pass_on(k, p, group, first, second, to_first, to_second):
        ref = codes[k].at[p, at(*turn(p, first, second))]
        send(ref, ref, k, 2, 4 + group, p, to_first, to_second)

    def wait_codes(k, group, count):
        wait(codes[k].at[:, pl.ds(0, count)], recv_sem.at[k, 4 + group])

    def first_stage(k):
        for d in (2, 1, 3):
            for p in range(2):
                pass_on(k, p, 1 if d == 2 else 0, 0, 0, d, 0)

    def second_stage(k, d):
        for p in range(2):
            for e in (1, 3):
                group = 2 if (e == 1) == (d < 2) else 3
                pass_on(k, p, group, d, 0, 0, e)

    def third_stage(k):
        wait_codes(k, 2, 4)
        for d in range(4):
            for p in range(2):
                e = 1 if d < 2 else 3
                pass_on(k, p, 4, d, 4 - e, 0, e)

    table = fraction_table((rows, 128))

    def finish(k, seconds):
        for p in range(2):
            for d in range(4):
                for e in seconds:
                    of_task = at(*turn(p, d, e))
                    for off in range(0, chunks[k], 128):
                        where = lanes(of_task, k, off, 128)
                        mean = decode(codes[k][p, of_task, :, off : off + 128], table)
                        out_ref[p, :, where] = base[p, :, where].astype(jnp.float32) + mean

    def enter(k):
        trim(k)
        if k == 0:
            pl.semaphore_wait(barrier, len(PEERS))
        send_bundles(k)

    def own_codes(k):
        second_stage(k, 0)

    def near_codes(k):
        wait_codes(k, 0, 2)
        second_stage(k, 3)
        second_stage(k, 1)

    def far_codes(k):
        wait_codes(k, 1, 1)
        second_stage(k, 2)

    def gather(k):
        reduce(k)
        first_stage(k)

    def finish_near(k):
        if k == 0:
            base_load.wait()
        wait_codes(k, 3, 4)
        finish(k, (0, 1, 3))

    def finish_far(k):
        wait_codes(k, 4, 4)
        finish(k, (2,))

    for load in loads:
        load.wait()
    for steps in (
        (enter,), (send_transit, send_direct), (merge,), (gather, own_codes), (near_codes, far_codes),
        (third_stage,), (finish_near,), (finish_far,),
    ):
        for k in range(kinds):
            for step in steps:
                step(k)
    for k in range(kinds):
        wait(bundles[k], send_sem.at[k, 0])
        wait(bundles[k], send_sem.at[k, 1])
        wait(codes[k].at[:, pl.ds(0, TASKS - 1)], send_sem.at[k, 2])


def on_device(deltas, keep_blocks, base_weights):
    halves, rows, columns = base_weights.shape
    share = columns // TASKS
    assert sum(CHUNKS) == share
    operands = [
        pltpu.with_memory_space_constraint(value, pltpu.HBM)
        for value in (keep_blocks, deltas, base_weights)
    ]
    return pl.pallas_call(
        functools.partial(kernel, CHUNKS),
        out_shape=jax.ShapeDtypeStruct((halves, rows, columns), jnp.float32),
        in_specs=[
            pl.BlockSpec(memory_space=pltpu.HBM),
            pl.BlockSpec(memory_space=pltpu.HBM),
            pl.BlockSpec(memory_space=pltpu.HBM),
        ],
        out_specs=pl.BlockSpec(memory_space=pltpu.VMEM),
        scratch_shapes=[
            pltpu.VMEM((halves, rows, columns), jnp.bfloat16),
            pltpu.VMEM((halves, rows, columns), jnp.bfloat16),
            pltpu.SMEM(keep_blocks.shape, jnp.int32),
            pltpu.SemaphoreType.DMA((4,)),
            pltpu.SemaphoreType.DMA((len(CHUNKS), SENDS)),
            pltpu.SemaphoreType.DMA((len(CHUNKS), RECEIVES)),
            *[pltpu.VMEM((halves, SIDE - 1, SIDE, rows, width), jnp.bfloat16) for width in CHUNKS],
            *[pltpu.VMEM((halves, SIDE, SIDE, rows, width), jnp.bfloat16) for width in CHUNKS],
            *[pltpu.VMEM((halves, 2, SIDE, HALF, width), jnp.bfloat16) for width in CHUNKS * 2],
            *[pltpu.VMEM((halves, 2, 4, HALF, width), jnp.int16) for width in CHUNKS * 2],
            *[pltpu.VMEM((halves, TASKS, rows, width), jnp.int16) for width in CHUNKS],
        ],
        compiler_params=pltpu.CompilerParams(
            collective_id=0, has_side_effects=True, vmem_limit_bytes=40 * 2**20
        ),
        name="merge",
    )(*operands)


def solution(mesh):
    in_specs = (P("task", None, "dp", "mp"), P("task", None, None), P(None, "dp", "mp"))
    out_specs = P(None, "dp", "mp")
    return jax.shard_map(
        on_device, mesh=mesh, in_specs=in_specs, out_specs=out_specs, check_vma=False
    )
```

```python
import functools

import jax
import jax.numpy as jnp
from jax import lax
from jax.experimental import pallas as pl
from jax.experimental.pallas import tpu as pltpu
from jax.sharding import PartitionSpec as P

BLOCK = 128
SIDE = 4
TASKS = SIDE * SIDE
MESH = pl.DeviceIdType.MESH

CHUNKS = (256, 256, 256, 128)
HALF = 16
PEERS = ((0, 2), (2, 0), (0, 1), (1, 0), (0, 3), (3, 0))
SENDS, RECEIVES = 3, 8

ORDER = (
    ("A", 0), ("A", 1), ("A", 2), ("A", 3), ("B", 1), ("B", 0), ("C", 1), ("B", 2), ("C", 0), ("B", 3),
    ("D", 1), ("D", 0), ("C", 2), ("D", 2), ("D", 3), ("C", 3), ("E", 1), ("E", 0), ("F", 0), ("F", 1),
    ("E", 2), ("F", 2), ("E", 3), ("G", 1), ("G", 0), ("H", 1), ("H", 0), ("G", 2), ("H", 2), ("G", 3),
    ("F", 3), ("H", 3), ("I", 1), ("J", 1), ("I", 0), ("I", 2), ("I", 3), ("J", 0), ("J", 3), ("J", 2),
    ("K", 0), ("K", 1), ("K", 2), ("K", 3),
)


def fraction_table(shape):
    j = lax.broadcasted_iota(jnp.int32, shape, 1)
    n = jnp.zeros(shape, jnp.int32)
    for m in range(1, 17):
        n = n + jnp.where(j >= m * (m - 1) // 2, 1, 0)
    r = j - n * (n - 1) // 2
    r = jnp.where(n == 16, 2 * r + 1, r)
    return r.astype(jnp.float32) / n.astype(jnp.float32)


def encode(upward, downward, up_count, down_count):
    total = upward + downward
    positive = total > 0.0
    amount = jnp.where(positive, upward, -downward) * 64.0
    count = jnp.where(positive, up_count, down_count) * 64.0
    n = jnp.maximum(count, 1.0)
    whole = jnp.floor(amount / n + 0.015625)
    r = amount - whole * n
    half = jnp.floor(r * 0.5)
    odd = r - 2.0 * half
    slot = n * (n - 1.0) * 0.5 + r
    slot16 = jnp.where(odd > 0.0, 120.0 + half, 28.0 + half)
    slot = jnp.where(n > 15.5, slot16, slot)
    code = whole * 128.0 + slot
    code = jnp.where(positive, code, jnp.where(total < 0.0, -code, 0.0))
    return code.astype(jnp.int32).astype(jnp.int16)


def decode(code, table):
    c = code.astype(jnp.int32)
    a = jnp.abs(c)
    whole = lax.shift_right_logical(a, 7).astype(jnp.float32)
    part = jnp.take_along_axis(table, a & 127, axis=1)
    mean = (whole + part) * 0.015625
    return jnp.where(c < 0, -mean, mean)


def tally(values, totals=None):
    for value in values:
        value = value.astype(jnp.float32)
        up, down = jnp.maximum(value, 0.0), jnp.minimum(value, 0.0)
        new = (up, down, jnp.minimum(up, 0.015625), -jnp.maximum(down, -0.015625))
        totals = new if totals is None else tuple(a + b for a, b in zip(totals, new))
    return totals


def kernel(chunks, keep_hbm, deltas_ref, base_ref, out_ref, own, base, keep_ref, load_sem, send_sem, recv_sem, *scratch):
    kinds = len(chunks)
    bundles, line, transit, direct, merged, partial, codes = (
        scratch[i * kinds : (i + 1) * kinds] for i in range(7)
    )
    rows, columns = own.shape[1], own.shape[2]
    share = columns // TASKS
    task = lax.axis_index("task")
    y, x = task // SIDE, task % SIDE
    block = lax.axis_index("dp") * rows // BLOCK
    halves = (slice(0, HALF), slice(HALF, rows))

    def at(dy, dx):
        return (y + dy) % SIDE * SIDE + (x + dx) % SIDE

    def turn(p, first, second):
        return (second, first) if p == 0 else (first, second)

    def place(p, second):
        return ((y, x)[p] + second) % SIDE

    starts = [sum(chunks[:k]) for k in range(kinds)]

    def lanes(of_task, k, off=0, width=None):
        start = pl.multiple_of(TASKS * starts[k] + of_task * chunks[k] + off, 128)
        return pl.ds(start, width or chunks[k])

    loads = []
    for k in range(kinds):
        part = pl.ds(TASKS * starts[k], TASKS * chunks[k])
        source, target = deltas_ref.at[0, :, :, part], own.at[:, :, part]
        loads.append(pltpu.make_async_copy(source, target, load_sem.at[k]))
    keep_load = pltpu.make_async_copy(keep_hbm, keep_ref, load_sem.at[kinds])
    base_load = pltpu.make_async_copy(base_ref, base, load_sem.at[kinds + 1])
    keep_load.start()
    for load in loads:
        load.start()

    barrier = pltpu.get_barrier_semaphore()
    for dy, dx in PEERS:
        pl.semaphore_signal(barrier, inc=1, device_id={"task": at(dy, dx)}, device_id_type=MESH)
    keep_load.wait()
    keeps = [keep_ref[0, p, block].astype(jnp.float32) for p in range(2)]

    def send(src, dst, k, send_slot, recv_slot, p, first, second):
        dy, dx = turn(p, first, second)
        pltpu.make_async_remote_copy(
            src_ref=src,
            dst_ref=dst,
            send_sem=send_sem.at[send_slot],
            recv_sem=recv_sem.at[k, recv_slot],
            device_id={"task": at(dy, dx)},
            device_id_type=MESH,
        ).start()

    def wait(ref, sem):
        pltpu.make_async_copy(ref, ref, sem).wait()

    def trim(k):
        for d in (2, 1, 3, 0):
            for p in range(2):
                for q in range(SIDE):
                    first = ((x, y)[p] + d) % SIDE
                    of_task = q * SIDE + first if p == 0 else first * SIDE + q
                    value = own[p, :, lanes(of_task, k)].astype(jnp.float32) * keeps[p]
                    if d:
                        bundles[k][p, d - 1, q] = value.astype(jnp.bfloat16)
                    else:
                        line[k][p, 0, q] = value.astype(jnp.bfloat16)

    def send_bundles(k):
        for d in (2, 1, 3):
            for p in range(2):
                send(bundles[k].at[p, d - 1], line[k].at[p, d], k, 0, 0, p, d, 0)

    def send_transit(k):
        wait(line[k].at[:, pl.ds(1, 3)], recv_sem.at[k, 0])
        for side, e in ((0, 1), (1, 3)):
            for p in range(2):
                far = line[k].at[p, :, place(p, 2), halves[side]]
                send(far, transit[k].at[p, side], k, 1, 1, p, 0, e)

    def send_direct(k):
        for side, e in ((0, 1), (1, 3)):
            for p in range(2):
                near = line[k].at[p, :, place(p, e), halves[1 - side]]
                send(near, direct[k].at[p, side], k, 1, 2, p, 0, e)

    def merge(k):
        wait(transit[k], recv_sem.at[k, 1])
        for side, e in ((0, 1), (1, 3)):
            for p in range(2):
                for off in range(0, chunks[k], 128):
                    tile = slice(off, off + 128)
                    values = [transit[k][p, side, j, :, tile] for j in range(SIDE)]
                    values += [line[k][p, j, place(p, e), halves[side], tile] for j in range(SIDE)]
                    for i, total in enumerate(tally(values)):
                        total = (total * 64.0).astype(jnp.int32).astype(jnp.int16)
                        merged[k][p, side, i, :, tile] = total
        for side, e in ((0, 1), (1, 3)):
            for p in range(2):
                send(merged[k].at[p, side], partial[k].at[p, side], k, 1, 2, p, 0, e)

    def reduce(k):
        wait(bundles[k].at[:, pl.ds(0, 2)], recv_sem.at[k, 2])
        for p in range(2):
            for side in range(2):
                for off in range(0, chunks[k], 128):
                    tile = slice(off, off + 128)
                    totals = tuple(
                        partial[k][p, side, i, :, tile].astype(jnp.int32).astype(jnp.float32) * 0.015625
                        for i in range(4)
                    )
                    values = [direct[k][p, 1 - side, j, :, tile] for j in range(SIDE)]
                    values += [line[k][p, j, place(p, 0), halves[side], tile] for j in range(SIDE)]
                    codes[k][p, task, halves[side], tile] = encode(*tally(values, totals))

    def pass_on(k, p, group, first, second, to_first, to_second):
        ref = codes[k].at[p, at(*turn(p, first, second))]
        send(ref, ref, k, 2, 3 + group, p, to_first, to_second)

    def wait_codes(k, group, count):
        wait(codes[k].at[:, pl.ds(0, count)], recv_sem.at[k, 3 + group])

    def first_stage(k):
        for d in (2, 1, 3):
            for p in range(2):
                pass_on(k, p, 1 if d == 2 else 0, 0, 0, d, 0)

    def second_stage(k, d):
        for p in range(2):
            for e in (1, 3):
                group = 2 if (e == 1) == (d < 2) else 3
                pass_on(k, p, group, d, 0, 0, e)

    def third_stage(k):
        wait_codes(k, 2, 4)
        for d in range(4):
            for p in range(2):
                e = 1 if d < 2 else 3
                pass_on(k, p, 4, d, 4 - e, 0, e)

    table = fraction_table((rows, 128))

    def finish(k, seconds):
        for p in range(2):
            for d in range(4):
                for e in seconds:
                    of_task = at(*turn(p, d, e))
                    for off in range(0, chunks[k], 128):
                        where = lanes(of_task, k, off, 128)
                        mean = decode(codes[k][p, of_task, :, off : off + 128], table)
                        out_ref[p, :, where] = base[p, :, where].astype(jnp.float32) + mean

    def enter(k):
        loads[k].wait()
        trim(k)
        if k == 0:
            pl.semaphore_wait(barrier, len(PEERS))
        if k == kinds - 1:
            base_load.start()
        send_bundles(k)

    def own_codes(k):
        second_stage(k, 0)

    def near_codes(k):
        wait_codes(k, 0, 2)
        second_stage(k, 3)
        second_stage(k, 1)

    def far_codes(k):
        wait_codes(k, 1, 1)
        second_stage(k, 2)

    def gather(k):
        reduce(k)
        first_stage(k)

    def finish_near(k):
        wait_codes(k, 3, 4)
        finish(k, (0, 1, 3))

    def finish_far(k):
        wait_codes(k, 4, 4)
        finish(k, (2,))

    stages = dict(
        A=enter, B=send_transit, C=send_direct, D=merge, E=gather, F=own_codes, G=near_codes, H=far_codes,
        I=third_stage, J=finish_near, K=finish_far,
    )
    first_finish = next(k for stage, k in ORDER if stage == "J")
    for stage, k in ORDER:
        if (stage, k) == ("J", first_finish):
            base_load.wait()
        stages[stage](k)
    for slot, pieces in ((0, TASKS - SIDE), (1, TASKS - SIDE), (2, TASKS - 1)):
        wait(own.at[:, :, pl.ds(0, pieces * share)], send_sem.at[slot])


def on_device(deltas, keep_blocks, base_weights):
    halves, rows, columns = base_weights.shape
    share = columns // TASKS
    assert sum(CHUNKS) == share
    operands = [
        pltpu.with_memory_space_constraint(value, pltpu.HBM)
        for value in (keep_blocks, deltas, base_weights)
    ]
    return pl.pallas_call(
        functools.partial(kernel, CHUNKS),
        out_shape=jax.ShapeDtypeStruct((halves, rows, columns), jnp.float32),
        in_specs=[
            pl.BlockSpec(memory_space=pltpu.HBM),
            pl.BlockSpec(memory_space=pltpu.HBM),
            pl.BlockSpec(memory_space=pltpu.HBM),
        ],
        out_specs=pl.BlockSpec(memory_space=pltpu.VMEM),
        scratch_shapes=[
            pltpu.VMEM((halves, rows, columns), jnp.bfloat16),
            pltpu.VMEM((halves, rows, columns), jnp.bfloat16),
            pltpu.SMEM(keep_blocks.shape, jnp.int32),
            pltpu.SemaphoreType.DMA((len(CHUNKS) + 2,)),
            pltpu.SemaphoreType.DMA((SENDS,)),
            pltpu.SemaphoreType.DMA((len(CHUNKS), RECEIVES)),
            *[pltpu.VMEM((halves, SIDE - 1, SIDE, rows, width), jnp.bfloat16) for width in CHUNKS],
            *[pltpu.VMEM((halves, SIDE, SIDE, rows, width), jnp.bfloat16) for width in CHUNKS],
            *[pltpu.VMEM((halves, 2, SIDE, HALF, width), jnp.bfloat16) for width in CHUNKS * 2],
            *[pltpu.VMEM((halves, 2, 4, HALF, width), jnp.int16) for width in CHUNKS * 2],
            *[pltpu.VMEM((halves, TASKS, rows, width), jnp.int16) for width in CHUNKS],
        ],
        compiler_params=pltpu.CompilerParams(
            collective_id=0, has_side_effects=True, vmem_limit_bytes=40 * 2**20
        ),
        name="merge",
    )(*operands)


def solution(mesh):
    in_specs = (P("task", None, "dp", "mp"), P("task", None, None), P(None, "dp", "mp"))
    out_specs = P(None, "dp", "mp")
    return jax.shard_map(
        on_device, mesh=mesh, in_specs=in_specs, out_specs=out_specs, check_vma=False
    )
```

```python
import functools

import jax
import jax.numpy as jnp
from jax import lax
from jax.experimental import pallas as pl
from jax.experimental.pallas import tpu as pltpu
from jax.sharding import PartitionSpec as P

BLOCK = 128
SIDE = 4
TASKS = SIDE * SIDE
MESH = pl.DeviceIdType.MESH

CHUNKS = (256, 256, 256, 128)
HALF = 16
PEERS = ((0, 2), (2, 0), (0, 1), (1, 0), (0, 3), (3, 0))
SENDS, RECEIVES = 3, 8

ORDER = (
    ("A", 0), ("A", 1), ("A", 2), ("A", 3), ("B", 1), ("B", 0), ("C", 1), ("B", 2), ("C", 0), ("B", 3),
    ("D", 1), ("D", 0), ("C", 2), ("D", 2), ("C", 3), ("D", 3), ("E", 1), ("F", 1), ("E", 0), ("F", 0),
    ("E", 2), ("E", 3), ("F", 2), ("G", 1), ("H", 1), ("G", 0), ("H", 0), ("G", 2), ("H", 2), ("H", 3),
    ("G", 3), ("F", 3), ("I", 1), ("I", 0), ("J", 0), ("I", 2), ("J", 2), ("I", 3), ("J", 3), ("J", 1),
    ("K", 0), ("K", 1), ("K", 2), ("K", 3),
)


def fraction_table(shape):
    j = lax.broadcasted_iota(jnp.int32, shape, 1)
    n = jnp.zeros(shape, jnp.int32)
    for m in range(1, 17):
        n = n + jnp.where(j >= m * (m - 1) // 2, 1, 0)
    r = j - n * (n - 1) // 2
    r = jnp.where(n == 16, 2 * r + 1, r)
    return r.astype(jnp.float32) / n.astype(jnp.float32)


def encode(upward, downward, up_count, down_count):
    total = upward + downward
    positive = total > 0.0
    amount = jnp.where(positive, upward, -downward) * 64.0
    count = jnp.where(positive, up_count, down_count) * 64.0
    n = jnp.maximum(count, 1.0)
    whole = jnp.floor(amount / n + 0.015625)
    r = amount - whole * n
    half = jnp.floor(r * 0.5)
    odd = r - 2.0 * half
    slot = n * (n - 1.0) * 0.5 + r
    slot16 = jnp.where(odd > 0.0, 120.0 + half, 28.0 + half)
    slot = jnp.where(n > 15.5, slot16, slot)
    code = whole * 128.0 + slot
    code = jnp.where(positive, code, jnp.where(total < 0.0, -code, 0.0))
    return code.astype(jnp.int32).astype(jnp.int16)


def decode(code, table):
    c = code.astype(jnp.int32)
    a = jnp.abs(c)
    whole = lax.shift_right_logical(a, 7).astype(jnp.float32)
    part = jnp.take_along_axis(table, a & 127, axis=1)
    mean = (whole + part) * 0.015625
    return jnp.where(c < 0, -mean, mean)


def tally(values, totals=None):
    for value in values:
        value = value.astype(jnp.float32)
        up, down = jnp.maximum(value, 0.0), jnp.minimum(value, 0.0)
        new = (up, down, jnp.minimum(up, 0.015625), -jnp.maximum(down, -0.015625))
        totals = new if totals is None else tuple(a + b for a, b in zip(totals, new))
    return totals


def kernel(chunks, keep_hbm, deltas_ref, base_ref, out_ref, own, base, keep_ref, load_sem, send_sem, recv_sem, *scratch):
    kinds = len(chunks)
    bundles, line, transit, direct, merged, partial, codes = (
        scratch[i * kinds : (i + 1) * kinds] for i in range(7)
    )
    rows, columns = own.shape[1], own.shape[2]
    share = columns // TASKS
    task = lax.axis_index("task")
    y, x = task // SIDE, task % SIDE
    block = lax.axis_index("dp") * rows // BLOCK
    halves = (slice(0, HALF), slice(HALF, rows))

    def at(dy, dx):
        return (y + dy) % SIDE * SIDE + (x + dx) % SIDE

    def turn(p, first, second):
        return (second, first) if p == 0 else (first, second)

    def place(p, second):
        return ((y, x)[p] + second) % SIDE

    starts = [sum(chunks[:k]) for k in range(kinds)]

    def lanes(of_task, k, off=0, width=None):
        start = pl.multiple_of(TASKS * starts[k] + of_task * chunks[k] + off, 128)
        return pl.ds(start, width or chunks[k])

    loads = []
    for k in range(kinds):
        part = pl.ds(TASKS * starts[k], TASKS * chunks[k])
        source, target = deltas_ref.at[0, :, :, part], own.at[:, :, part]
        loads.append(pltpu.make_async_copy(source, target, load_sem.at[k]))
    keep_load = pltpu.make_async_copy(keep_hbm, keep_ref, load_sem.at[kinds])
    base_load = pltpu.make_async_copy(base_ref, base, load_sem.at[kinds + 1])
    keep_load.start()
    for load in loads:
        load.start()

    barrier = pltpu.get_barrier_semaphore()
    for dy, dx in PEERS:
        pl.semaphore_signal(barrier, inc=1, device_id={"task": at(dy, dx)}, device_id_type=MESH)
    keep_load.wait()
    keeps = [keep_ref[0, p, block].astype(jnp.float32) for p in range(2)]

    def send(src, dst, k, send_slot, recv_slot, p, first, second):
        dy, dx = turn(p, first, second)
        pltpu.make_async_remote_copy(
            src_ref=src,
            dst_ref=dst,
            send_sem=send_sem.at[send_slot],
            recv_sem=recv_sem.at[k, recv_slot],
            device_id={"task": at(dy, dx)},
            device_id_type=MESH,
        ).start()

    def wait(ref, sem):
        pltpu.make_async_copy(ref, ref, sem).wait()

    def trim(k):
        for d in (2, 1, 3, 0):
            for p in range(2):
                for q in range(SIDE):
                    first = ((x, y)[p] + d) % SIDE
                    of_task = q * SIDE + first if p == 0 else first * SIDE + q
                    value = own[p, :, lanes(of_task, k)].astype(jnp.float32) * keeps[p]
                    if d:
                        bundles[k][p, d - 1, q] = value.astype(jnp.bfloat16)
                    else:
                        line[k][p, 0, q] = value.astype(jnp.bfloat16)

    def send_bundles(k):
        for d in (2, 1, 3):
            for p in range(2):
                send(bundles[k].at[p, d - 1], line[k].at[p, d], k, 0, 0, p, d, 0)

    def send_transit(k):
        wait(line[k].at[:, pl.ds(1, 3)], recv_sem.at[k, 0])
        for side, e in ((0, 1), (1, 3)):
            for p in range(2):
                far = line[k].at[p, :, place(p, 2), halves[side]]
                send(far, transit[k].at[p, side], k, 1, 1, p, 0, e)

    def send_direct(k):
        for side, e in ((0, 1), (1, 3)):
            for p in range(2):
                near = line[k].at[p, :, place(p, e), halves[1 - side]]
                send(near, direct[k].at[p, side], k, 1, 2, p, 0, e)

    def merge(k):
        wait(transit[k], recv_sem.at[k, 1])
        for side, e in ((0, 1), (1, 3)):
            for p in range(2):
                for off in range(0, chunks[k], 128):
                    tile = slice(off, off + 128)
                    values = [transit[k][p, side, j, :, tile] for j in range(SIDE)]
                    values += [line[k][p, j, place(p, e), halves[side], tile] for j in range(SIDE)]
                    for i, total in enumerate(tally(values)):
                        total = (total * 64.0).astype(jnp.int32).astype(jnp.int16)
                        merged[k][p, side, i, :, tile] = total
        for side, e in ((0, 1), (1, 3)):
            for p in range(2):
                send(merged[k].at[p, side], partial[k].at[p, side], k, 1, 2, p, 0, e)

    def reduce(k):
        wait(bundles[k].at[:, pl.ds(0, 2)], recv_sem.at[k, 2])
        for p in range(2):
            for side in range(2):
                for off in range(0, chunks[k], 128):
                    tile = slice(off, off + 128)
                    totals = tuple(
                        partial[k][p, side, i, :, tile].astype(jnp.int32).astype(jnp.float32) * 0.015625
                        for i in range(4)
                    )
                    values = [direct[k][p, 1 - side, j, :, tile] for j in range(SIDE)]
                    values += [line[k][p, j, place(p, 0), halves[side], tile] for j in range(SIDE)]
                    codes[k][p, task, halves[side], tile] = encode(*tally(values, totals))

    def pass_on(k, p, group, first, second, to_first, to_second):
        ref = codes[k].at[p, at(*turn(p, first, second))]
        send(ref, ref, k, 2, 3 + group, p, to_first, to_second)

    def wait_codes(k, group, count):
        wait(codes[k].at[:, pl.ds(0, count)], recv_sem.at[k, 3 + group])

    def first_stage(k):
        for d in (2, 1, 3):
            for p in range(2):
                pass_on(k, p, 1 if d == 2 else 0, 0, 0, d, 0)

    def second_stage(k, d):
        for p in range(2):
            for e in (1, 3):
                group = 2 if (e == 1) == (d < 2) else 3
                pass_on(k, p, group, d, 0, 0, e)

    def third_stage(k):
        wait_codes(k, 2, 4)
        for d in range(4):
            for p in range(2):
                e = 1 if d < 2 else 3
                pass_on(k, p, 4, d, 4 - e, 0, e)

    table = fraction_table((rows, 128))

    def finish(k, seconds):
        for p in range(2):
            for d in range(4):
                for e in seconds:
                    of_task = at(*turn(p, d, e))
                    for off in range(0, chunks[k], 128):
                        where = lanes(of_task, k, off, 128)
                        mean = decode(codes[k][p, of_task, :, off : off + 128], table)
                        out_ref[p, :, where] = base[p, :, where].astype(jnp.float32) + mean

    def enter(k):
        loads[k].wait()
        trim(k)
        if k == 0:
            pl.semaphore_wait(barrier, len(PEERS))
        if k == kinds - 1:
            base_load.start()
        send_bundles(k)

    def own_codes(k):
        second_stage(k, 0)

    def near_codes(k):
        wait_codes(k, 0, 2)
        second_stage(k, 3)
        second_stage(k, 1)

    def far_codes(k):
        wait_codes(k, 1, 1)
        second_stage(k, 2)

    def gather(k):
        reduce(k)
        first_stage(k)

    def finish_near(k):
        wait_codes(k, 3, 4)
        finish(k, (0, 1, 3))

    def finish_far(k):
        wait_codes(k, 4, 4)
        finish(k, (2,))

    stages = dict(
        A=enter, B=send_transit, C=send_direct, D=merge, E=gather, F=own_codes, G=near_codes, H=far_codes,
        I=third_stage, J=finish_near, K=finish_far,
    )
    first_finish = next(k for stage, k in ORDER if stage == "J")
    for stage, k in ORDER:
        if (stage, k) == ("J", first_finish):
            base_load.wait()
        stages[stage](k)
    for slot, pieces in ((0, TASKS - SIDE), (1, TASKS - SIDE), (2, TASKS - 1)):
        wait(own.at[:, :, pl.ds(0, pieces * share)], send_sem.at[slot])


def on_device(deltas, keep_blocks, base_weights):
    halves, rows, columns = base_weights.shape
    share = columns // TASKS
    assert sum(CHUNKS) == share
    operands = [
        pltpu.with_memory_space_constraint(value, pltpu.HBM)
        for value in (keep_blocks, deltas, base_weights)
    ]
    return pl.pallas_call(
        functools.partial(kernel, CHUNKS),
        out_shape=jax.ShapeDtypeStruct((halves, rows, columns), jnp.float32),
        in_specs=[
            pl.BlockSpec(memory_space=pltpu.HBM),
            pl.BlockSpec(memory_space=pltpu.HBM),
            pl.BlockSpec(memory_space=pltpu.HBM),
        ],
        out_specs=pl.BlockSpec(memory_space=pltpu.VMEM),
        scratch_shapes=[
            pltpu.VMEM((halves, rows, columns), jnp.bfloat16),
            pltpu.VMEM((halves, rows, columns), jnp.bfloat16),
            pltpu.SMEM(keep_blocks.shape, jnp.int32),
            pltpu.SemaphoreType.DMA((len(CHUNKS) + 2,)),
            pltpu.SemaphoreType.DMA((SENDS,)),
            pltpu.SemaphoreType.DMA((len(CHUNKS), RECEIVES)),
            *[pltpu.VMEM((halves, SIDE - 1, SIDE, rows, width), jnp.bfloat16) for width in CHUNKS],
            *[pltpu.VMEM((halves, SIDE, SIDE, rows, width), jnp.bfloat16) for width in CHUNKS],
            *[pltpu.VMEM((halves, 2, SIDE, HALF, width), jnp.bfloat16) for width in CHUNKS * 2],
            *[pltpu.VMEM((halves, 2, 4, HALF, width), jnp.int16) for width in CHUNKS * 2],
            *[pltpu.VMEM((halves, TASKS, rows, width), jnp.int16) for width in CHUNKS],
        ],
        compiler_params=pltpu.CompilerParams(
            collective_id=0, has_side_effects=True, vmem_limit_bytes=40 * 2**20
        ),
        name="merge",
    )(*operands)


def solution(mesh):
    in_specs = (P("task", None, "dp", "mp"), P("task", None, None), P(None, "dp", "mp"))
    out_specs = P(None, "dp", "mp")
    return jax.shard_map(
        on_device, mesh=mesh, in_specs=in_specs, out_specs=out_specs, check_vma=False
    )
```
